32 devices in a mesh: row: 2 (over x), col: 4 (over y, core), layer: 4 (over z).
Axes of the slice: x: 2, y: 2, z: 4, core: 2. Of those that a mesh axis runs over, the one named last changes fastest.
Arguments:
- panel: float32 [1024, 8192], P('layer', ('col', 'row')), may hold values from -0.75 to 0.75
- c_in: float32 [4, 2, 1024, 8192], P('layer', 'row', None, 'col'), may hold values from -1.5 to 1.5
Outputs:
- updated: float32 [4, 2, 1024, 8192], P('layer', 'row', None, 'col')
The draws below stay inside these ranges and needn't reach their ends.
All inputs are finite; a program needn't handle non-finite values.
Results may differ from the reference program's by a relative error of at most 0.000062.
Values sent between devices are 32-bit elements; how exact they have to be, the bound alone decides.
No kernel may reach another device: no remote copies, remote signals or barrier semaphores. Data moves between devices by JAX's collectives and lax.ppermute only.
A program may use at most 128 MiB of HBM per device.

```python
import jax
import jax.numpy as jnp
from jax import lax

N = 8192
K = 1024
W = 1024
N_ROW = 2
N_COL = 4


def steps_of(stream_key, extent, pieces, smallest, largest):
    level = 1.0
    for position, parts in pieces:
        draws = jax.random.uniform(jax.random.fold_in(jax.random.fold_in(stream_key, 6), position), (parts,), jnp.float32, smallest / len(pieces), largest / len(pieces))
        level = level * jnp.repeat(jnp.exp(draws), extent[position] // parts).reshape((-1,) + (1,) * (len(extent) - 1 - position))
    return level


def noise(key, shape, spread, limit, shards=(), held_as=jnp.bfloat16):
    values = spread * jax.random.normal(key, shape, jnp.float32)
    if shards:
        values = values * steps_of(key, shape, shards, -0.22, 0.18)
    return jnp.clip(values, -limit, limit).astype(held_as)


def setup_inputs(seed: int = 0) -> dict:
    arg_keys = jax.random.split(jax.random.key(seed), 3)
    return {
        "panel": noise(arg_keys[0], (K, N), (0.3 * K ** -0.25), 0.75, ((0, 4), (1, 8)), jnp.float32),
        "c_in": noise(arg_keys[1], (N_COL, N_ROW, W, N), 0.1, 1.5, ((0, 4), (1, 2), (3, 4)), jnp.float32),
    }


def reference(panel, c_in):
    gram = lax.dot_general(panel, panel, (((0,), (0,)), ((), ())), precision=lax.Precision.HIGHEST, preferred_element_type=jnp.float32)
    gram = gram.reshape(N_COL, N_ROW, N // (N_ROW * N_COL), N)
    return c_in + gram
```

```python
import functools

import jax
import jax.numpy as jnp
from jax import lax
from jax.experimental import pallas as pl
from jax.experimental.pallas import tpu as pltpu
from jax.sharding import PartitionSpec as P

AXES = ("row", "col", "layer")
F32, BF16 = jnp.float32, jnp.bfloat16
VMEM = pl.BlockSpec(memory_space=pltpu.VMEM)
SMEM = pl.BlockSpec(memory_space=pltpu.SMEM)
ANY = pl.BlockSpec(memory_space=pl.ANY)


def split(x):
    high = x.astype(BF16)
    return high, (x - high.astype(F32)).astype(BF16)


def stacked_left(x):
    high, low = split(x)
    return jnp.concatenate([high, high, low], 0)


def stacked_right(x):
    high, low = split(x)
    return jnp.concatenate([high, low, high], 0)


def dot(left, right):
    return lax.dot_general(left, right, (((0,), (0,)), ((), ())), preferred_element_type=F32)


def params(mib):
    return pltpu.CompilerParams(vmem_limit_bytes=mib << 20, has_side_effects=True)


def cost(flops):
    return pl.CostEstimate(flops=flops, bytes_accessed=1 << 20, transcendentals=0)


def call(kernel, args, outs, aliases=None, scratch=(), flops=1 << 20, mib=40):
    return pl.pallas_call(
        kernel,
        in_specs=[spec for _, spec in args],
        out_specs=[spec for _, spec in outs],
        out_shape=[shape for shape, _ in outs],
        input_output_aliases=aliases or {},
        scratch_shapes=scratch,
        compiler_params=params(mib),
        cost_estimate=cost(flops),
    )(*(a for a, _ in args))


def load_acc(flags, c, own, other, sems):
    width = own.shape[1]
    row = flags[0]
    copies = [
        pltpu.make_async_copy(c.at[:, pl.ds(pl.multiple_of(row * width, width), width)], own, sems.at[0]),
        pltpu.make_async_copy(c.at[:, pl.ds(pl.multiple_of((1 - row) * width, width), width)], other, sems.at[1]),
    ]
    for copy in copies:
        copy.start()
    for copy in copies:
        copy.wait()


def choose(which, flags, *refs):
    flag = flags[which] == 1
    n = len(refs) // 3
    for a, b, out in zip(refs[:n], refs[n : 2 * n], refs[2 * n :], strict=True):

        @pl.when(flag)
        def _():
            out[...] = a[...]

        @pl.when(jnp.logical_not(flag))
        def _():
            out[...] = b[...]


def select(which, flags, firsts, seconds):
    shapes = [(pltpu.VMEM(a.shape, F32), VMEM) for a in firsts]
    args = [(flags, SMEM)] + [(a, VMEM) for a in (*firsts, *seconds)]
    return call(functools.partial(choose, which), args, shapes, mib=8)


def pick(flag, a, b):
    return lax.select(jnp.full(a.shape, flag), a, b)


class Pieces:
    def __init__(self, firsts, which=None, seconds=()):
        self.firsts, self.which, self.seconds = tuple(firsts), which, tuple(seconds)

    @property
    def arrays(self):
        return self.firsts + self.seconds

    def reader(self, flags, refs):
        firsts, seconds = refs[: len(self.firsts)], refs[len(self.firsts) :]

        def read(columns=slice(None)):
            def rows(group):
                parts = [r[:, columns] for r in group]
                return parts[0] if len(parts) == 1 else jnp.concatenate(parts, 0)

            if self.which is None:
                return rows(firsts)
            return pick(flags[self.which] == 1, rows(firsts), rows(seconds))

        return read


def accumulate(flags, terms, accs, tile=256):
    operands = [p for left, rights in terms for p in (left, *rights)]
    n_acc = len(accs)

    def kernel(flag_ref, *refs):
        at = 0
        readers = []
        for p in operands:
            readers.append(p.reader(flag_ref, refs[at : at + len(p.arrays)]))
            at += len(p.arrays)
        olds, news = refs[at : at + n_acc], refs[at + n_acc :]
        at = 0
        for left, rights in terms:
            stack = stacked_left(readers[at]())
            for i in range(n_acc):
                for j in range(0, olds[i].shape[1], tile):
                    cols = slice(j, j + tile)
                    base = olds[i] if at == 0 else news[i]
                    news[i][:, cols] = base[:, cols] + dot(stack, stacked_right(readers[at + 1 + i](cols)))
            at += 1 + n_acc

    arrays = [a for p in operands for a in p.arrays]
    args = [(flags, SMEM)] + [(a, VMEM) for a in arrays] + [(a, VMEM) for a in accs]
    outs = [(pltpu.VMEM(a.shape, F32), VMEM) for a in accs]
    first = 1 + len(arrays)
    flops = sum(6 * l.arrays[0].shape[0] * a.shape[0] * a.shape[1] for l, _ in terms for a in accs)
    return call(kernel, args, outs, {first + i: i for i in range(n_acc)}, flops=flops)


def finish(flags, terms, acc, half, shape, so_far=None, tile=256):
    operands = [p for left, right in terms for p in (left, right)]
    tiles = acc.shape[1] // tile

    def kernel(flag_ref, *refs):
        readers = []
        at = 0
        for p in operands:
            readers.append(p.reader(flag_ref, refs[at : at + len(p.arrays)]))
            at += len(p.arrays)
        old = refs[at]
        out, stack = refs[-2], refs[-1]
        j = pl.program_id(0)

        @pl.when(j == 0)
        def _():
            rows = 0
            for i in range(0, len(readers), 2):
                left = stacked_left(readers[i]())
                stack[rows : rows + left.shape[0]] = left
                rows += left.shape[0]

        cols = pl.ds(pl.multiple_of(j * tile, tile), tile)
        rights = [stacked_right(readers[i](cols)) for i in range(1, len(readers), 2)]
        right = rights[0] if len(rights) == 1 else jnp.concatenate(rights, 0)
        out[...] = old[:, cols] + dot(stack[...], right)

    arrays = [a for p in operands for a in p.arrays]
    args = arrays + [acc] + ([] if so_far is None else [so_far])
    specs = [VMEM] * (len(arrays) + 1) + ([] if so_far is None else [ANY])
    depth = sum(3 * sum(a.shape[0] for a in left.firsts) for left, _ in terms)
    return pl.pallas_call(
        kernel,
        grid_spec=pltpu.PrefetchScalarGridSpec(
            num_scalar_prefetch=1,
            grid=(tiles,),
            in_specs=specs,
            out_specs=pl.BlockSpec((acc.shape[0], tile), lambda j, flag_ref: (0, flag_ref[half] * tiles + j)),
            scratch_shapes=[pltpu.VMEM((depth, acc.shape[0]), BF16)],
        ),
        out_shape=jax.ShapeDtypeStruct(shape, F32),
        input_output_aliases={} if so_far is None else {len(args): 0},
        compiler_params=params(40),
        cost_estimate=cost(2 * depth * acc.shape[0] * acc.shape[1]),
    )(flags, *args)


def paired(mesh, panel, c_in):
    n_row, n_col, n_layer = (mesh.shape[a] for a in AXES)

    def send(x, to):
        pairs = []
        for r in range(n_row):
            for c in range(n_col):
                for l in range(n_layer):
                    target = to(r, c, l)
                    if target is not None:
                        a, b, d = target
                        pairs.append(((r * n_col + c) * n_layer + l, (a * n_col + b) * n_layer + d))
        return lax.ppermute(x, AXES, pairs)

    inner = lambda l: l in (1, 2)
    near = lambda r, c, l: (r, c, l ^ 1)
    outward = lambda r, c, l: (r, c, l ^ 1) if inner(l) else None
    middle = lambda r, c, l: (r, c, 3 - l) if inner(l) else None
    swap = lambda r, c, l: (1 - r, c, l)
    swap_ends = lambda r, c, l: None if inner(l) else (1 - r, c, l)
    across = lambda r, c, l: (r, c ^ 2, l) if c == l else None
    beside = lambda r, c, l: (r, c ^ 1, l) if c in (l, l ^ 2) else None

    row, col, layer = (lax.axis_index(a) for a in AXES)
    is_inner = (layer == 1) | (layer == 2)
    is_source = col == layer
    is_holder = is_source | (col == layer ^ 2)
    flags = jnp.stack([row, 1 - row, is_inner, is_source, is_holder]).astype(jnp.int32)
    INNER, SOURCE, HOLDER = 2, 3, 4

    depth, width = panel.shape
    half = depth // 2
    c_flat = c_in.reshape(c_in.shape[2:])
    p0a, p0b = panel[:half], panel[half:]

    a1a = send(p0a, near)
    x1 = send(panel, swap)
    b1a = send(p0a, middle)
    y0 = send(panel, across)
    a1b = send(p0b, near)
    b1b = send(p0b, middle)

    acc = [(pltpu.VMEM((c_flat.shape[0], width), F32), VMEM)] * 2
    own, other = call(load_acc, [(flags, SMEM), (c_flat, ANY)], acc, scratch=[pltpu.SemaphoreType.DMA((2,))], mib=20)

    a2a = send(b1a, outward)
    x2a = send(a1a, swap)
    b2a = send(a1a, middle)
    y1a = send(a1a, across)
    (m_0,) = select(SOURCE, flags, [panel], [y0])
    d0 = send(m_0, beside)

    a2b = send(b1b, outward)
    x2b = send(a1b, swap)
    b2b = send(a1b, middle)
    y1b = send(a1b, across)

    l0 = Pieces([m_0], HOLDER, [d0])
    own, other = accumulate(flags, [(l0, [Pieces([panel]), Pieces([x1])])], [own, other])

    a3a = send(b2a, outward)
    (s3a,) = select(INNER, flags, [b2a], [a2a])
    x3a = send(s3a, swap)
    m_1a, m_1b = select(SOURCE, flags, [a1a, a1b], [y1a, y1b])
    d1a = send(m_1a, beside)
    d1b = send(m_1b, beside)

    a3b = send(b2b, outward)
    s3b, p2a, p2b = select(INNER, flags, [b2b, b1a, b1b], [a2b, a2a, a2b])
    x3b = send(s3b, swap)
    y2a = send(p2a, across)
    y2b = send(p2b, across)
    b3 = send(x1, middle)

    l1 = Pieces([m_1a, m_1b], HOLDER, [d1a, d1b])
    own, other = accumulate(flags, [(l1, [Pieces([a1a, a1b]), Pieces([x2a, x2b])])], [own, other])

    a4 = send(x3a, outward)
    (p3a,) = select(INNER, flags, [b2a], [a3a])
    y3a = send(p3a, across)
    m_2a, m_2b = select(SOURCE, flags, [p2a, p2b], [y2a, y2b])
    d2a = send(m_2a, beside)
    d2b = send(m_2b, beside)

    x4 = send(a3b, swap_ends)
    (p3b,) = select(INNER, flags, [b2b], [a3b])
    y3b = send(p3b, across)
    (m_3a,) = select(SOURCE, flags, [p3a], [y3a])
    d3a = send(m_3a, beside)

    l2 = Pieces([m_2a, m_2b], HOLDER, [d2a, d2b])
    q2 = Pieces([b3], INNER, [x3a, x3b])
    q2 = Pieces([b3[:half], b3[half:]], INNER, [x3a, x3b]) if False else q2
    own, other = accumulate(flags, [(l2, [Pieces([p2a, p2b]), q2])], [own, other])

    (m_3b,) = select(SOURCE, flags, [p3b], [y3b])
    d3b = send(m_3b, beside)
    l3 = Pieces([m_3a, m_3b], HOLDER, [d3a, d3b])
    out = finish(flags, [(l3, Pieces([p3a, p3b]))], own, 0, c_flat.shape)
    q3 = Pieces([x3a, x3b], INNER, [a4, x4])
    out = finish(flags, [(l3, q3)], other, 1, c_flat.shape, out)
    return out.reshape(c_in.shape)


def gathered(panel, c_in):
    rows_here, width = c_in.shape[0], panel.shape[1]
    own = lax.all_gather(panel, "layer", axis=0, tiled=True)
    right = lax.all_gather(own, "row", axis=1, tiled=True)
    columns = lax.all_gather(own, "col", axis=0)
    mine = lax.dynamic_slice_in_dim(columns, lax.axis_index("layer") * rows_here, rows_here, 0)
    left = jnp.moveaxis(mine, 0, 1).reshape(own.shape[0], rows_here * width)
    tile = lax.dot_general(
        left, right, (((0,), (0,)), ((), ())), precision=lax.Precision.HIGHEST, preferred_element_type=F32
    )
    return c_in + tile.reshape(c_in.shape)


def solution(mesh):
    placed = (P("layer", ("col", "row")), P("layer", "row", None, "col"))
    fits = tuple(mesh.shape[a] for a in AXES) == (2, 4, 4)

    def on_device(panel, c_in):
        if not fits:
            return gathered(panel, c_in)
        return paired(mesh, panel, c_in)

    return jax.shard_map(
        on_device,
        mesh=mesh,
        in_specs=placed,
        out_specs=P("layer", "row", None, "col"),
        check_vma=False,
    )
```

```python
import jax
import jax.numpy as jnp
from jax import lax
from jax.experimental import pallas as pl
from jax.experimental.pallas import tpu as pltpu
from jax.sharding import PartitionSpec as P

AXES = ("row", "col", "layer")
F32, BF16 = jnp.float32, jnp.bfloat16
VMEM = pl.BlockSpec(memory_space=pltpu.VMEM)
SMEM = pl.BlockSpec(memory_space=pltpu.SMEM)
HBM = pl.BlockSpec(memory_space=pltpu.HBM)
ANY = pl.BlockSpec(memory_space=pl.ANY)
SUM_MIB, FINISH_MIB = 16, 24


def split(x):
    high = x.astype(BF16)
    return high, (x - high.astype(F32)).astype(BF16)


def left_stack(x):
    high, low = split(x)
    return jnp.concatenate([high, high, low], 0)


def right_stack(x):
    high, low = split(x)
    return jnp.concatenate([high, low, high], 0)


def dot(left, right):
    return lax.dot_general(left, right, (((0,), (0,)), ((), ())), preferred_element_type=F32)


def params(mib):
    return pltpu.CompilerParams(vmem_limit_bytes=mib << 20, has_side_effects=True)


def cost(flops):
    return pl.CostEstimate(flops=flops, bytes_accessed=1 << 20, transcendentals=0)


def call(kernel, args, outs, aliases=None, scratch=(), flops=1 << 20, mib=40):
    return pl.pallas_call(
        kernel,
        in_specs=[spec for _, spec in args],
        out_specs=[spec for _, spec in outs],
        out_shape=[shape for shape, _ in outs],
        input_output_aliases=aliases or {},
        scratch_shapes=scratch,
        compiler_params=params(mib),
        cost_estimate=cost(flops),
    )(*(a for a, _ in args))


def load(flags, c, own, other, sems):
    width = own.shape[1]
    row = flags[0]
    halves = [(row, own, 0), (1 - row, other, 1)]
    copies = [
        pltpu.make_async_copy(c.at[:, pl.ds(pl.multiple_of(i * width, width), width)], to, sems.at[k])
        for i, to, k in halves
    ]
    for copy in copies:
        copy.start()
    for copy in copies:
        copy.wait()


def mark(flags, out):
    out[...] = jnp.full(out.shape, flags[0])


def part(x, first, second):
    at = first.shape[0]
    first[...] = x[:at]
    second[...] = x[at:]


def select(which, flags, firsts, seconds):
    windows = [s if isinstance(s, tuple) else (s, 0) for s in seconds]
    n = len(firsts)

    def kernel(flag_ref, *refs):
        outs = refs[2 * n :]

        @pl.when(flag_ref[which] == 1)
        def _():
            for source, out in zip(refs[:n], outs, strict=True):
                out[...] = source[...]

        @pl.when(flag_ref[which] != 1)
        def _():
            for source, (_, start), out in zip(refs[n : 2 * n], windows, outs, strict=True):
                out[...] = source[start : start + out.shape[0]]

    outs = [(pltpu.VMEM(a.shape, F32), VMEM) for a in firsts]
    args = [(flags, SMEM)] + [(a, VMEM) for a in (*firsts, *(a for a, _ in windows))]
    return call(kernel, args, outs, mib=8)


class Operand:
    def __init__(self, *groups):
        listed = lambda c: c if isinstance(c, tuple) else (c,)
        self.groups = [(g[0], [listed(c) for c in g[1]]) if isinstance(g, tuple) else (None, [(g,)]) for g in groups]
        self.rows = sum(a.shape[0] for _, choices in self.groups for a in choices[0])
        self.arrays = [a for _, choices in self.groups for c in choices for a in c]
        self.plain = len(self.arrays) == 1

    def scratch(self, width):
        return [] if self.plain else [pltpu.VMEM((self.rows, width), F32)]

    def settle(self, flags, refs, scratch):
        if self.plain:
            return refs.pop(0)
        to, start = scratch.pop(0), 0
        for which, choices in self.groups:
            for i, arrays in enumerate(choices):
                sources = [refs.pop(0) for _ in arrays]

                def copy(sources=sources, row=start):
                    for source in sources:
                        to[row : row + source.shape[0]] = source[...]
                        row += source.shape[0]

                copy() if which is None else pl.when(flags[which] == i)(copy)
            start += sum(a.shape[0] for a in choices[0])
        return to


def accumulate(flags, left, rights, accs, tile=256):
    n = len(accs)
    operands = [left, *rights]
    arrays = [a for p in operands for a in p.arrays]
    width = accs[0].shape[1]

    def kernel(flag_ref, *refs):
        refs, olds, rest = list(refs[: len(arrays)]), refs[len(arrays) :][:n], refs[len(arrays) + n :]
        news, scratch = rest[:n], list(rest[n:])
        held = [p.settle(flag_ref, refs, scratch) for p in operands]
        stack = left_stack(held[0][...])
        for i in range(n):
            for j in range(0, width, tile):
                cols = slice(j, j + tile)
                news[i][:, cols] = olds[i][:, cols] + dot(stack, right_stack(held[1 + i][:, cols]))

    args = [(flags, SMEM)] + [(a, VMEM) for a in arrays] + [(a, VMEM) for a in accs]
    outs = [(pltpu.VMEM(a.shape, F32), VMEM) for a in accs]
    first = 1 + len(arrays)
    scratch = [s for p in operands for s in p.scratch(width)]
    flops = sum(6 * left.rows * a.shape[0] * a.shape[1] for a in accs)
    return call(kernel, args, outs, {first + i: i for i in range(n)}, scratch, flops=flops, mib=SUM_MIB)


def finish(flags, left, rights, accs, halves, shape, tile=128):
    operands = [left, *rights]
    arrays = [a for p in operands for a in p.arrays]
    height, width = accs[0].shape
    tiles, n = height // tile, len(accs)

    def kernel(flag_ref, *refs):
        olds, rest = refs[len(arrays) :][:n], list(refs[len(arrays) + n :])
        out, ready, sems = rest[0], rest[-2], rest[-1]
        refs, scratch = list(refs[: len(arrays)]), rest[1:-2]
        held = [p.settle(flag_ref, refs, scratch) for p in operands]
        stack = left_stack(held[0][...])
        copies = []
        for k in range(n):
            right = right_stack(held[1 + k][...])
            cols = pl.ds(pl.multiple_of(flag_ref[halves[k]] * width, width), width)
            for i in range(tiles):
                rows = slice(i * tile, (i + 1) * tile)
                ready[k, rows] = olds[k][rows] + dot(stack[:, rows], right)
                copies.append(pltpu.make_async_copy(ready.at[k, rows], out.at[rows, cols], sems.at[k, i]))
                copies[-1].start()
        for copy in copies:
            copy.wait()

    args = [(flags, SMEM)] + [(a, VMEM) for a in arrays] + [(a, VMEM) for a in accs]
    scratch = [s for p in operands for s in p.scratch(width)]
    scratch += [pltpu.VMEM((n, height, width), F32), pltpu.SemaphoreType.DMA((n, tiles))]
    flops = 6 * left.rows * height * width * n
    (out,) = call(kernel, args, [(jax.ShapeDtypeStruct(shape, F32), ANY)], scratch=scratch, flops=flops, mib=FINISH_MIB)
    return out


def paired(mesh, panel, c_in):
    n_row, n_col, n_layer = (mesh.shape[a] for a in AXES)

    def send(x, to):
        pairs = []
        for r in range(n_row):
            for c in range(n_col):
                for l in range(n_layer):
                    target = to(r, c, l)
                    if target is not None:
                        a, b, d = target
                        pairs.append(((r * n_col + c) * n_layer + l, (a * n_col + b) * n_layer + d))
        return lax.ppermute(x, AXES, pairs)

    inner = lambda l: l in (1, 2)
    near = lambda r, c, l: (r, c, l ^ 1)
    outward = lambda r, c, l: (r, c, l ^ 1) if inner(l) else None
    middle = lambda r, c, l: (r, c, 3 - l) if inner(l) else None
    swap = lambda r, c, l: (1 - r, c, l)
    swap_ends = lambda r, c, l: None if inner(l) else (1 - r, c, l)
    across = lambda r, c, l: (r, c ^ 2, l) if c == l else None
    beside = lambda r, c, l: (r, c ^ 1, l) if c == l else None
    beyond = lambda r, c, l: (r, c ^ 1, l) if c == l ^ 2 else None

    row, col, layer = (lax.axis_index(a) for a in AXES)
    place = col ^ layer
    flags = jnp.stack([row, 1 - row, (layer == 1) | (layer == 2), place == 0, place & 1, place]).astype(jnp.int32)
    ROW, OTHER_ROW, INNER, _, _, PLACE = range(6)

    depth, width = panel.shape
    cut = depth * CUT // 16
    c_flat = c_in.reshape(c_in.shape[2:])

    b1 = send(panel, middle)
    a1 = send(panel, near)
    x1 = send(panel, swap)
    y0 = send(panel, across)
    acc = [(pltpu.VMEM((c_flat.shape[0], width), F32), VMEM)] * 2
    own, other = call(load, [(flags, SMEM), (c_flat, HBM)], acc, scratch=[pltpu.SemaphoreType.DMA((2,))], mib=20)
    e0 = send(panel, beside)
    f0 = send(y0, beyond)

    a2 = send(b1, outward)
    call(mark, [(flags, SMEM)], [(pltpu.VMEM((8, 128), jnp.int32), VMEM)], mib=1)
    parts = [(pltpu.VMEM((n, width), F32), VMEM) for n in (cut, depth - cut)]
    p1a, p1b = call(part, [(a1, VMEM)], parts, mib=8)
    b2a = send(p1a, middle)
    x2 = send(a1, swap)
    b2b = send(p1b, middle)
    y1 = send(a1, across)
    e1 = send(a1, beside)
    b3 = send(x1, middle)
    left = Operand((PLACE, (panel, e0, y0, f0)))
    own, other = accumulate(flags, left, [Operand(panel), Operand(x1)], [own, other])

    a3a = send(b2a, outward)
    f1 = send(y1, beyond)
    (s3a,) = select(INNER, flags, [b2a], [a2])
    x3a = send(s3a, swap)
    a3b = send(b2b, outward)
    s3b, p2 = select(INNER, flags, [b2b, b1], [(a2, cut), a2])
    x3b = send(s3b, swap)
    y2 = send(p2, across)
    e2 = send(p2, beside)
    left = Operand((PLACE, (a1, e1, y1, f1)))
    own, other = accumulate(flags, left, [Operand(a1), Operand(x2)], [own, other])

    (p3a,) = select(INNER, flags, [b2a], [a3a])
    y3a = send(p3a, across)
    e3a = send(p3a, beside)
    a4 = send(x3a, outward)
    f2 = send(y2, beyond)
    (p3b,) = select(INNER, flags, [b2b], [a3b])
    y3b = send(p3b, across)
    x4 = send(a3b, swap_ends)
    e3b = send(p3b, beside)
    f3a = send(y3a, beyond)
    f3b = send(y3b, beyond)
    left = Operand((PLACE, (p2, e2, y2, f2)))
    q2 = Operand((INNER, ((x3a, x3b), (b3,))))
    own, other = accumulate(flags, left, [Operand(p2), q2], [own, other])
    left = Operand((PLACE, ((p3a, p3b), (e3a, e3b), (y3a, y3b), (f3a, f3b))))
    q3 = Operand((INNER, (a4, x3a)), (INNER, (x4, x3b)))
    halves = [ROW, OTHER_ROW]
    out = finish(flags, left, [Operand(p3a, p3b), q3], [own, other], halves, c_flat.shape)
    return out.reshape(c_in.shape)


CUT = 10


def gathered(panel, c_in):
    rows_here, width = c_in.shape[0], panel.shape[1]
    own = lax.all_gather(panel, "layer", axis=0, tiled=True)
    right = lax.all_gather(own, "row", axis=1, tiled=True)
    columns = lax.all_gather(own, "col", axis=0)
    mine = lax.dynamic_slice_in_dim(columns, lax.axis_index("layer") * rows_here, rows_here, 0)
    left = jnp.moveaxis(mine, 0, 1).reshape(own.shape[0], rows_here * width)
    tile = lax.dot_general(
        left, right, (((0,), (0,)), ((), ())), precision=lax.Precision.HIGHEST, preferred_element_type=F32
    )
    return c_in + tile.reshape(c_in.shape)


def solution(mesh):
    placed = (P("layer", ("col", "row")), P("layer", "row", None, "col"))
    fits = tuple(mesh.shape[a] for a in AXES) == (2, 4, 4)

    def on_device(panel, c_in):
        if not fits:
            return gathered(panel, c_in)
        return paired(mesh, panel, c_in)

    return jax.shard_map(
        on_device,
        mesh=mesh,
        in_specs=placed,
        out_specs=P("layer", "row", None, "col"),
        check_vma=False,
    )
```

```python
import jax
import jax.numpy as jnp
from jax import lax
from jax.experimental import pallas as pl
from jax.experimental.pallas import tpu as pltpu
from jax.sharding import PartitionSpec as P

AXES = ("row", "col", "layer")
F32, BF16 = jnp.float32, jnp.bfloat16
VMEM = pl.BlockSpec(memory_space=pltpu.VMEM)
SMEM = pl.BlockSpec(memory_space=pltpu.SMEM)
HBM = pl.BlockSpec(memory_space=pltpu.HBM)
ANY = pl.BlockSpec(memory_space=pl.ANY)
SUM_MIB, FINISH_MIB = 16, 24


def split(x):
    high = x.astype(BF16)
    return high, (x - high.astype(F32)).astype(BF16)


def left_stack(x):
    high, low = split(x)
    return jnp.concatenate([high, high, low], 0)


def right_stack(x):
    high, low = split(x)
    return jnp.concatenate([high, low, high], 0)


def dot(left, right):
    return lax.dot_general(left, right, (((0,), (0,)), ((), ())), preferred_element_type=F32)


def params(mib):
    return pltpu.CompilerParams(vmem_limit_bytes=mib << 20, has_side_effects=True)


def cost(flops):
    return pl.CostEstimate(flops=flops, bytes_accessed=1 << 20, transcendentals=0)


def call(kernel, args, outs, aliases=None, scratch=(), flops=1 << 20, mib=40):
    return pl.pallas_call(
        kernel,
        in_specs=[spec for _, spec in args],
        out_specs=[spec for _, spec in outs],
        out_shape=[shape for shape, _ in outs],
        input_output_aliases=aliases or {},
        scratch_shapes=scratch,
        compiler_params=params(mib),
        cost_estimate=cost(flops),
    )(*(a for a, _ in args))


def load(flags, c, own, other, sems):
    width = own.shape[1]
    row = flags[0]
    halves = [(row, own, 0), (1 - row, other, 1)]
    copies = [
        pltpu.make_async_copy(c.at[:, pl.ds(pl.multiple_of(i * width, width), width)], to, sems.at[k])
        for i, to, k in halves
    ]
    for copy in copies:
        copy.start()
    for copy in copies:
        copy.wait()


def part(x, first, second):
    at = first.shape[0]
    first[...] = x[:at]
    second[...] = x[at:]


def select(which, flags, firsts, seconds):
    windows = [s if isinstance(s, tuple) else (s, 0) for s in seconds]
    n = len(firsts)

    def kernel(flag_ref, *refs):
        outs = refs[2 * n :]

        @pl.when(flag_ref[which] == 1)
        def _():
            for source, out in zip(refs[:n], outs, strict=True):
                out[...] = source[...]

        @pl.when(flag_ref[which] != 1)
        def _():
            for source, (_, start), out in zip(refs[n : 2 * n], windows, outs, strict=True):
                out[...] = source[start : start + out.shape[0]]

    outs = [(pltpu.VMEM(a.shape, F32), VMEM) for a in firsts]
    args = [(flags, SMEM)] + [(a, VMEM) for a in (*firsts, *(a for a, _ in windows))]
    return call(kernel, args, outs, mib=8)


class Operand:
    def __init__(self, *groups):
        listed = lambda c: c if isinstance(c, tuple) else (c,)
        self.groups = [(g[0], [listed(c) for c in g[1]]) if isinstance(g, tuple) else (None, [(g,)]) for g in groups]
        self.rows = sum(a.shape[0] for _, choices in self.groups for a in choices[0])
        self.arrays = [a for _, choices in self.groups for c in choices for a in c]
        self.plain = len(self.arrays) == 1

    def scratch(self, width):
        return [] if self.plain else [pltpu.VMEM((self.rows, width), F32)]

    def settle(self, flags, refs, scratch):
        if self.plain:
            return refs.pop(0)
        to, start = scratch.pop(0), 0
        for which, choices in self.groups:
            for i, arrays in enumerate(choices):
                sources = [refs.pop(0) for _ in arrays]

                def copy(sources=sources, row=start):
                    for source in sources:
                        to[row : row + source.shape[0]] = source[...]
                        row += source.shape[0]

                copy() if which is None else pl.when(flags[which] == i)(copy)
            start += sum(a.shape[0] for a in choices[0])
        return to


def accumulate(flags, left, rights, accs, tile=256):
    n = len(accs)
    operands = [left, *rights]
    arrays = [a for p in operands for a in p.arrays]
    width = accs[0].shape[1]

    def kernel(flag_ref, *refs):
        refs, olds, rest = list(refs[: len(arrays)]), refs[len(arrays) :][:n], refs[len(arrays) + n :]
        news, scratch = rest[:n], list(rest[n:])
        held = [p.settle(flag_ref, refs, scratch) for p in operands]
        stack = left_stack(held[0][...])
        for i in range(n):
            for j in range(0, width, tile):
                cols = slice(j, j + tile)
                news[i][:, cols] = olds[i][:, cols] + dot(stack, right_stack(held[1 + i][:, cols]))

    args = [(flags, SMEM)] + [(a, VMEM) for a in arrays] + [(a, VMEM) for a in accs]
    outs = [(pltpu.VMEM(a.shape, F32), VMEM) for a in accs]
    first = 1 + len(arrays)
    scratch = [s for p in operands for s in p.scratch(width)]
    flops = sum(6 * left.rows * a.shape[0] * a.shape[1] for a in accs)
    return call(kernel, args, outs, {first + i: i for i in range(n)}, scratch, flops=flops, mib=SUM_MIB)


def finish(flags, left, rights, accs, halves, shape, tile=256):
    operands = [left, *rights]
    arrays = [a for p in operands for a in p.arrays]
    height, width = accs[0].shape
    tiles, n = height // tile, len(accs)

    def kernel(flag_ref, *refs):
        olds, rest = refs[len(arrays) :][:n], list(refs[len(arrays) + n :])
        out, ready, sems = rest[0], rest[-2], rest[-1]
        refs, scratch = list(refs[: len(arrays)]), rest[1:-2]
        held = [p.settle(flag_ref, refs, scratch) for p in operands]
        stack = left_stack(held[0][...])
        copies = []
        for k in range(n):
            right = right_stack(held[1 + k][...])
            cols = pl.ds(pl.multiple_of(flag_ref[halves[k]] * width, width), width)
            for i in range(tiles):
                rows = slice(i * tile, (i + 1) * tile)
                ready[k, rows] = olds[k][rows] + dot(stack[:, rows], right)
                copies.append(pltpu.make_async_copy(ready.at[k, rows], out.at[rows, cols], sems.at[k, i]))
                copies[-1].start()
        for copy in copies:
            copy.wait()

    args = [(flags, SMEM)] + [(a, VMEM) for a in arrays] + [(a, VMEM) for a in accs]
    scratch = [s for p in operands for s in p.scratch(width)]
    scratch += [pltpu.VMEM((n, height, width), F32), pltpu.SemaphoreType.DMA((n, tiles))]
    flops = 6 * left.rows * height * width * n
    (out,) = call(kernel, args, [(jax.ShapeDtypeStruct(shape, F32), ANY)], scratch=scratch, flops=flops, mib=FINISH_MIB)
    return out


def paired(mesh, panel, c_in):
    n_row, n_col, n_layer = (mesh.shape[a] for a in AXES)

    def send(x, to):
        pairs = []
        for r in range(n_row):
            for c in range(n_col):
                for l in range(n_layer):
                    target = to(r, c, l)
                    if target is not None:
                        a, b, d = target
                        pairs.append(((r * n_col + c) * n_layer + l, (a * n_col + b) * n_layer + d))
        return lax.ppermute(x, AXES, pairs)

    inner = lambda l: l in (1, 2)
    near = lambda r, c, l: (r, c, l ^ 1)
    outward = lambda r, c, l: (r, c, l ^ 1) if inner(l) else None
    middle = lambda r, c, l: (r, c, 3 - l) if inner(l) else None
    swap = lambda r, c, l: (1 - r, c, l)
    swap_ends = lambda r, c, l: None if inner(l) else (1 - r, c, l)
    across = lambda r, c, l: (r, c ^ 2, l) if c == l else None
    beside = lambda r, c, l: (r, c ^ 1, l) if c == l else None
    beyond = lambda r, c, l: (r, c ^ 1, l) if c == l ^ 2 else None

    row, col, layer = (lax.axis_index(a) for a in AXES)
    place = col ^ layer
    flags = jnp.stack([row, 1 - row, (layer == 1) | (layer == 2), place == 0, place & 1, place]).astype(jnp.int32)
    ROW, OTHER_ROW, INNER, _, _, PLACE = range(6)

    depth, width = panel.shape
    cut = depth * CUT // 16
    c_flat = c_in.reshape(c_in.shape[2:])

    b1 = send(panel, middle)
    a1 = send(panel, near)
    x1 = send(panel, swap)
    y0 = send(panel, across)
    acc = [(pltpu.VMEM((c_flat.shape[0], width), F32), VMEM)] * 2
    own, other = call(load, [(flags, SMEM), (c_flat, HBM)], acc, scratch=[pltpu.SemaphoreType.DMA((2,))], mib=20)
    e0 = send(panel, beside)
    f0 = send(y0, beyond)

    a2 = send(b1, outward)
    parts = [(pltpu.VMEM((n, width), F32), VMEM) for n in (cut, depth - cut)]
    p1a, p1b = call(part, [(a1, VMEM)], parts, mib=8)
    b2a = send(p1a, middle)
    x2 = send(a1, swap)
    y1 = send(a1, across)
    b2b = send(p1b, middle)
    e1 = send(a1, beside)
    left = Operand((PLACE, (panel, e0, y0, f0)))
    own, other = accumulate(flags, left, [Operand(panel), Operand(x1)], [own, other])

    a3a = send(b2a, outward)
    f1 = send(y1, beyond)
    b3 = send(x1, middle)
    s3a, p2 = select(INNER, flags, [b2a, b1], [a2, a2])
    x3a = send(s3a, swap)
    y2 = send(p2, across)
    a3b = send(b2b, outward)
    (s3b,) = select(INNER, flags, [b2b], [(a2, cut)])
    x3b = send(s3b, swap)
    e2 = send(p2, beside)
    left = Operand((PLACE, (a1, e1, y1, f1)))
    own, other = accumulate(flags, left, [Operand(a1), Operand(x2)], [own, other])

    (p3a,) = select(INNER, flags, [b2a], [a3a])
    y3a = send(p3a, across)
    e3a = send(p3a, beside)
    a4 = send(x3a, outward)
    f2 = send(y2, beyond)
    (p3b,) = select(INNER, flags, [b2b], [a3b])
    y3b = send(p3b, across)
    x4 = send(a3b, swap_ends)
    e3b = send(p3b, beside)
    f3a = send(y3a, beyond)
    f3b = send(y3b, beyond)
    left = Operand((PLACE, (p2, e2, y2, f2)))
    q2 = Operand((INNER, ((x3a, x3b), (b3,))))
    own, other = accumulate(flags, left, [Operand(p2), q2], [own, other])
    left = Operand((PLACE, ((p3a, p3b), (e3a, e3b), (y3a, y3b), (f3a, f3b))))
    q3 = Operand((INNER, (a4, x3a)), (INNER, (x4, x3b)))
    halves = [ROW, OTHER_ROW]
    out = finish(flags, left, [Operand(p3a, p3b), q3], [own, other], halves, c_flat.shape)
    return out.reshape(c_in.shape)


CUT = 10


def gathered(panel, c_in):
    rows_here, width = c_in.shape[0], panel.shape[1]
    own = lax.all_gather(panel, "layer", axis=0, tiled=True)
    right = lax.all_gather(own, "row", axis=1, tiled=True)
    columns = lax.all_gather(own, "col", axis=0)
    mine = lax.dynamic_slice_in_dim(columns, lax.axis_index("layer") * rows_here, rows_here, 0)
    left = jnp.moveaxis(mine, 0, 1).reshape(own.shape[0], rows_here * width)
    tile = lax.dot_general(
        left, right, (((0,), (0,)), ((), ())), precision=lax.Precision.HIGHEST, preferred_element_type=F32
    )
    return c_in + tile.reshape(c_in.shape)


def solution(mesh):
    placed = (P("layer", ("col", "row")), P("layer", "row", None, "col"))
    fits = tuple(mesh.shape[a] for a in AXES) == (2, 4, 4)

    def on_device(panel, c_in):
        if not fits:
            return gathered(panel, c_in)
        return paired(mesh, panel, c_in)

    return jax.shard_map(
        on_device,
        mesh=mesh,
        in_specs=placed,
        out_specs=P("layer", "row", None, "col"),
        check_vma=False,
    )
```
